32 devices in a mesh: groups: 2 (over x), rows: 16 (over z, y, core).
Axes of the slice: x: 2, y: 2, z: 4, core: 2. Of those that a mesh axis runs over, the one named last changes fastest.
Arguments:
- bin_ids: int32 [16384, 512], P(('groups', 'rows')), parts along dimension 0, may hold values from 0 to 255
- gradients: bfloat16 [16384], P(('groups', 'rows')), parts along dimension 0, may hold values from -6 to 6
- hessians: bfloat16 [16384], P(('groups', 'rows')), parts along dimension 0, may hold values from 0.049804688 to 1
- node_ids: int32 [16384], P(('groups', 'rows')), parts along dimension 0, may hold values from 0 to 15
- predictions: float32 [16384], P(('groups', 'rows')), parts along dimension 0, may hold values from -6 to 6
- split_feature: int32 [32], P('groups'), parts along dimension 0, may hold values from 0 to 511
- split_bin: int32 [32], P('groups'), parts along dimension 0, may hold values from 0 to 254
Outputs:
- gains: float32 [1024, 16, 256], P(('groups', 'rows')), parts along dimension 0
- best_gain: float32 [32], P('groups'), parts along dimension 0
- leaf_values: float32 [2, 32], P(None, 'groups'), parts along dimension 1
- new_predictions: float32 [16384], P(('groups', 'rows')), parts along dimension 0
The draws below stay inside these ranges and needn't reach their ends.
There are 2 independent parts, one for each index of `groups`. The reference program is written for one: setup_inputs(seed, part) draws one part's arguments, and reference() takes and returns one part's arrays. A program takes and returns all parts, laid end to end along the dimension named above; each array names one. Nothing has to cross between parts.
All inputs are finite; a program needn't handle non-finite values.
Results may differ from the reference program's by a relative error of at most 0.0003.
Values sent between devices are 32-bit elements; how exact they have to be, the bound alone decides.
No kernel may reach another device: no remote copies, remote signals or barrier semaphores. Data moves between devices by JAX's collectives and lax.ppermute only.
A program may use at most 64 MiB of HBM per device.

```python
import math
import jax
import jax.numpy as jnp
import numpy as np

F = 512
BINS = 256
NODES = 16
ROWS = 8192


def with_ends(result, own_key, least, high):
    index_at = [jax.random.randint(jax.random.fold_in(own_key, axis), (), 0, length) for axis, length in enumerate(result.shape)]
    widest = result.shape.index(max(result.shape))
    neighbour = index_at[:widest] + [(index_at[widest] + 1) % result.shape[widest]] + index_at[widest + 1:]
    return result.at[tuple(index_at)].set(least).at[tuple(neighbour)].set(high)


def block_levels(stream_key, extent, pieces, smallest, largest):
    def one(dim, parts):
        heights = jax.random.uniform(jax.random.fold_in(jax.random.fold_in(stream_key, 6), dim), (parts,), jnp.float32, smallest / len(pieces), largest / len(pieces))
        return jnp.repeat(jnp.exp(heights), extent[dim] // parts).reshape((-1,) + (1,) * (len(extent) - dim - 1))

    loudness = one(*pieces[0])
    for cut in pieces[1:]:
        loudness = loudness * one(*cut)
    return loudness


def rank_table(amount, skew):
    weights = [(1 << 20) // math.isqrt(standing ** skew) + 1 for standing in range(1, amount + 1)]
    deviation = 1 + sum(weights) // (1 << 30)
    return np.cumsum(np.array([max(1, weight // deviation) for weight in weights]))


def skewed_ids(key, shape, amount, slope):
    grid = rank_table(amount, slope)
    ticket = jax.random.randint(jax.random.fold_in(key, 1), shape, 0, int(grid[amount - 1]))
    rank = jnp.searchsorted(jnp.asarray(grid, jnp.int32), ticket, side="right")
    return jax.random.permutation(jax.random.fold_in(key, 2), amount)[rank].astype(jnp.int32)


def gaussian(key, extent, scale, most, pieces=(), kind=jnp.bfloat16):
    result = jax.random.normal(key, extent, jnp.float32) * scale
    if len(pieces) > 0:
        result = block_levels(key, extent, pieces, -0.22, 0.18) * result
    return jnp.clip(result, min=-most, max=most).astype(kind)


def setup_inputs(seed: int = 0, part: int = 0) -> dict:
    splits = jax.random.split(jax.random.key(seed), 8)
    part_splits = jax.random.split(jax.random.fold_in(splits[7], part), 8)
    bin_ids = with_ends(jax.random.randint(part_splits[0], (ROWS, F), 0, BINS), jax.random.fold_in(part_splits[0], 1), 0, BINS - 1).astype(jnp.int32)
    gradients = gaussian(part_splits[1], (ROWS,), 1.0, 6.0, ((0, 16),))
    hessians = jnp.clip(jnp.exp(math.log(1.0) - 2.9996462 * jax.random.uniform(part_splits[2], (ROWS,), jnp.float32) ** block_levels(part_splits[2], (ROWS,), ((0, 16),), -0.2, 0.2)), 0.049804688, 1.0).astype(jnp.bfloat16)
    node_ids = with_ends(skewed_ids(part_splits[3], (ROWS,), NODES, 2), jax.random.fold_in(part_splits[3], 3), 0, NODES - 1).astype(jnp.int32)
    predictions = gaussian(part_splits[4], (ROWS,), 1.0, 6.0, ((0, 16),), jnp.float32)
    split_feature = with_ends(jax.random.randint(part_splits[5], (NODES,), 0, F), jax.random.fold_in(part_splits[5], 1), 0, F - 1).astype(jnp.int32)
    split_bin = with_ends(jax.random.randint(part_splits[6], (NODES,), 0, BINS - 1), jax.random.fold_in(part_splits[6], 1), 0, (BINS - 1) - 1).astype(jnp.int32)
    return {"bin_ids": bin_ids, "gradients": gradients, "hessians": hessians, "node_ids": node_ids, "predictions": predictions, "split_feature": split_feature, "split_bin": split_bin}


l2_penalty = 1.0
shrinkage = 0.5


def histogram_of(values, slot_ids, shape_like):
    spread = jnp.broadcast_to(values.astype(jnp.float32)[:, None], shape_like).reshape(-1)
    summed = jax.ops.segment_sum(spread, slot_ids, num_segments=NODES * F * BINS)
    return summed.reshape(NODES, F, BINS).transpose(1, 0, 2)


def reference(bin_ids, gradients, hessians, node_ids, predictions, split_feature, split_bin):
    feature_base = jnp.arange(F, dtype=jnp.int32) * BINS
    slot_ids = (node_ids[:, None] * (F * BINS) + feature_base[None, :] + bin_ids).astype(jnp.int32).reshape(-1)
    hist_grad = histogram_of(gradients, slot_ids, bin_ids.shape)
    hist_hess = histogram_of(hessians, slot_ids, bin_ids.shape)
    cum_grad = jnp.cumsum(hist_grad, axis=2)
    cum_hess = jnp.cumsum(hist_hess, axis=2)
    tot_grad = cum_grad[:, :, -1:]
    tot_hess = cum_hess[:, :, -1:]
    gains = 0.5 * (cum_grad ** 2 / (cum_hess + l2_penalty)
                   + (tot_grad - cum_grad) ** 2 / (tot_hess - cum_hess + l2_penalty)
                   - tot_grad ** 2 / (tot_hess + l2_penalty))
    best_gain = jnp.max(gains, axis=(0, 2))
    node_range = jnp.arange(NODES, dtype=jnp.int32)
    left_grad = cum_grad[split_feature, node_range, split_bin]
    left_hess = cum_hess[split_feature, node_range, split_bin]
    node_grad = tot_grad[split_feature, node_range, 0]
    node_hess = tot_hess[split_feature, node_range, 0]
    leaf_left = -left_grad / (left_hess + l2_penalty)
    leaf_right = -(node_grad - left_grad) / (node_hess - left_hess + l2_penalty)
    leaf_values = jnp.stack([leaf_left, leaf_right])
    row_feature = split_feature[node_ids]
    row_bin = jnp.take_along_axis(bin_ids, row_feature[:, None], axis=1)[:, 0]
    go_right = row_bin > split_bin[node_ids]
    new_predictions = predictions + shrinkage * jnp.where(go_right, leaf_right[node_ids], leaf_left[node_ids])
    return gains, best_gain, leaf_values, new_predictions
```

```python
import functools

import jax
import jax.numpy as jnp
from jax import lax
from jax.experimental import pallas as pl
from jax.experimental.pallas import tpu as pltpu
from jax.sharding import PartitionSpec as P

BINS = 256
NODES = 16
LANES = 128
HALF = BINS // 2
EXTRA = 4

l2_penalty = 1.0
shrinkage = 0.5

VMEM = pl.BlockSpec(memory_space=pltpu.VMEM)


def prep_kernel(bins_ref, info_ref, node_ref, split_ref, pay_ref):
    peers, _, _ = pay_ref.shape
    rows, feats = bins_ref.shape
    owned = feats // peers
    chunks = rows // LANES
    node_col = lax.broadcasted_iota(jnp.int32, (NODES, LANES), 0)
    feat_pos = lax.broadcasted_iota(jnp.int32, (NODES, feats), 1)
    pick = jnp.where(feat_pos == split_ref[:, 0:1], 1.0, 0.0).astype(jnp.bfloat16)
    for c in range(chunks):
        block = bins_ref[c * LANES : (c + 1) * LANES, :].astype(jnp.float32)
        picked = lax.dot_general(
            pick,
            block.astype(jnp.bfloat16),
            (((1,), (1,)), ((), ())),
            preferred_element_type=jnp.float32,
        )
        member = node_ref[c : c + 1, :] == node_col
        right = picked > split_ref[:, 1:2].astype(jnp.float32)
        side = jnp.sum(jnp.where(member & right, 1.0, 0.0), axis=0, keepdims=True)
        flipped = block.T
        info = [info_ref[k, c : c + 1, :] for k in range(3)] + [side]
        for d in range(peers):
            pay_ref[d, c * owned : (c + 1) * owned, :] = flipped[d * owned : (d + 1) * owned, :]
            for k in range(EXTRA):
                at = chunks * owned + k * chunks + c
                pay_ref[d, at : at + 1, :] = info[k]


def hist_kernel(pay_ref, mine_ref, pred_ref, gains_ref, best_ref, leaf_ref, new_ref, w_ref):
    peers = pay_ref.shape[0]
    owned = gains_ref.shape[0]
    chunks = pred_ref.shape[0]
    base = chunks * owned
    bf16 = jnp.bfloat16
    node_col = lax.broadcasted_iota(jnp.int32, (NODES, LANES), 0).astype(jnp.float32)

    def build(s, sums):
        out = list(sums)
        for c in range(chunks):
            g, h, node, side = (
                pay_ref[s, base + k * chunks + c : base + k * chunks + c + 1, :]
                for k in range(EXTRA)
            )
            member = node == node_col
            wg = jnp.where(member, g, 0.0)
            wh = jnp.where(member, h, 0.0)
            w_ref[s, c] = jnp.concatenate([wg, wh], axis=0).astype(bf16)
            left = side < 0.5
            out[0] = out[0] + jnp.where(left, wg, 0.0)
            out[1] = out[1] + jnp.where(left, wh, 0.0)
            out[2] = out[2] + wg
            out[3] = out[3] + wh
        return tuple(out)

    zero = jnp.zeros((NODES, LANES), jnp.float32)
    sums = lax.fori_loop(0, peers, build, (zero,) * 4)
    left_grad, left_hess, node_grad, node_hess = (
        jnp.sum(x, axis=1, keepdims=True) for x in sums
    )
    leaf_left = -left_grad / (left_hess + l2_penalty)
    leaf_right = -(node_grad - left_grad) / (node_hess - left_hess + l2_penalty)
    lane = lax.broadcasted_iota(jnp.int32, (NODES, LANES), 1)
    both = jnp.where(lane == 0, leaf_left, leaf_right)
    both = jnp.concatenate([both, jnp.zeros((LANES - NODES, LANES), jnp.float32)], axis=0)
    leaf_ref[...] = both.T[0:2, 0:NODES]
    for c in range(chunks):
        node = mine_ref[2 * chunks + c : 2 * chunks + c + 1, :]
        side = mine_ref[3 * chunks + c : 3 * chunks + c + 1, :]
        value = jnp.where(side < 0.5, leaf_left, leaf_right)
        value = jnp.sum(jnp.where(node == node_col, value, 0.0), axis=0, keepdims=True)
        new_ref[c : c + 1, :] = pred_ref[c : c + 1, :] + shrinkage * value

    row16 = lax.broadcasted_iota(jnp.int32, (16, LANES), 0)
    steps = [(row16 + 16 * i).astype(jnp.float32).astype(bf16) for i in range(HALF // 16)]
    one = jnp.ones((16, LANES), bf16)
    nil = jnp.zeros((16, LANES), bf16)

    def terms(s, c, f):
        row = jnp.broadcast_to(pay_ref[s, pl.ds(c * owned + f, 1), :], (8, LANES))
        high = jnp.where(row >= HALF, 1.0, 0.0)
        low = row - HALF * high
        low16 = jnp.concatenate([low, low], axis=0).astype(bf16)
        high16 = jnp.concatenate([high, high], axis=0).astype(bf16)
        rhs = jnp.concatenate([jnp.where(low16 <= t, one, nil) for t in steps], axis=0)
        first = one - high16
        w = w_ref[s, c]
        wg, wh = w[:NODES], w[NODES:]
        lhs = jnp.concatenate([wg * first, wh * first, wg * high16, wh * high16], axis=0)
        return lhs, rhs

    unroll = min(peers, 8)

    def scan(acc):
        def quad(q, best):
            def sources(j, carry):
                for u in range(unroll):
                    s = j * unroll + u
                    for t in range(chunks // 2):
                        for m in range(2):
                            f = q * 4 + m * 2
                            part = [[terms(s, 2 * t + i, f + e) for i in range(2)] for e in range(2)]
                            lhs = jnp.concatenate(
                                [jnp.concatenate([p[0] for p in e], axis=1) for e in part], axis=0
                            )
                            rhs = jnp.concatenate(
                                [jnp.concatenate([p[1] for p in e], axis=1) for e in part], axis=0
                            )
                            reg = (u * (chunks // 2) + t) % 2
                            pltpu.matmul_push_rhs(
                                rhs, staging_register=reg, mxu_index=m, transpose=True
                            )
                            pltpu.matmul_acc_lhs(acc[m], lhs, load_staged_rhs=reg)
                return carry

            lax.fori_loop(0, peers // unroll, sources, 0)
            for m in range(2):
                out = pltpu.matmul_pop(acc[m])
                for e in range(2):
                    c = out[e * 64 : (e + 1) * 64, e * HALF : (e + 1) * HALF]
                    cums = []
                    for k in range(2):
                        a, b = c[k * 16 : (k + 1) * 16], c[32 + k * 16 : 48 + k * 16]
                        cums.append(jnp.concatenate([a, b + a[:, HALF - 1 : HALF]], axis=1))
                    cum_grad, cum_hess = cums
                    tot_grad = cum_grad[:, BINS - 1 : BINS]
                    tot_hess = cum_hess[:, BINS - 1 : BINS]
                    gain = 0.5 * (
                        cum_grad * cum_grad / (cum_hess + l2_penalty)
                        + (tot_grad - cum_grad) ** 2 / (tot_hess - cum_hess + l2_penalty)
                        - tot_grad * tot_grad / (tot_hess + l2_penalty)
                    )
                    gains_ref[q * 4 + m * 2 + e] = gain
                    best = jnp.maximum(best, gain)
            return best

        for m in range(2):
            pltpu.matmul_pop(acc[m])
        best = lax.fori_loop(
            0, owned // 4, quad, jnp.full((NODES, BINS), -jnp.inf, jnp.float32)
        )
        best = jnp.maximum(best[:, :LANES], best[:, LANES:])
        best = jnp.concatenate([best, jnp.zeros((LANES - NODES, LANES), jnp.float32)], axis=0)
        best_ref[...] = jnp.max(best.T, axis=0, keepdims=True)

    pl.run_scoped(
        lambda a, b: scan((a, b)),
        pltpu.ACC(0)((4 * 2 * NODES, BINS), jnp.float32),
        pltpu.ACC(1)((4 * 2 * NODES, BINS), jnp.float32),
    )


def body(mesh, bin_ids, gradients, hessians, node_ids, predictions, split_feature, split_bin):
    peers = mesh.shape["rows"]
    rows, feats = bin_ids.shape
    owned = feats // peers
    chunks = rows // LANES
    info = jnp.stack(
        [
            gradients.astype(jnp.float32),
            hessians.astype(jnp.float32),
            node_ids.astype(jnp.float32),
        ]
    ).reshape(3, chunks, LANES)
    split = jnp.stack([split_feature, split_bin], axis=1)
    depth = chunks * (owned + EXTRA)
    pay = pl.pallas_call(
        prep_kernel,
        out_shape=jax.ShapeDtypeStruct((peers, depth, LANES), jnp.float32),
        in_specs=[VMEM] * 4,
        out_specs=VMEM,
        name="prep",
    )(bin_ids, info, node_ids.reshape(chunks, LANES), split)
    got = lax.all_to_all(pay, "rows", 0, 0, tiled=True)
    mine = pay[0, chunks * owned :, :]
    gains, best, leaf_values, new_predictions = pl.pallas_call(
        hist_kernel,
        out_shape=(
            jax.ShapeDtypeStruct((owned, NODES, BINS), jnp.float32),
            jax.ShapeDtypeStruct((1, LANES), jnp.float32),
            jax.ShapeDtypeStruct((2, NODES), jnp.float32),
            jax.ShapeDtypeStruct((chunks, LANES), jnp.float32),
        ),
        in_specs=[VMEM] * 3,
        out_specs=(VMEM,) * 4,
        scratch_shapes=[pltpu.VMEM((peers, chunks, 2 * NODES, LANES), jnp.bfloat16)],
        name="hist",
    )(got, mine, predictions.reshape(chunks, LANES))
    spread = lax.all_to_all(
        jnp.broadcast_to(best, (peers, LANES)), "rows", 0, 0, tiled=True
    )
    best_gain = jnp.max(spread, axis=0)[:NODES]
    return gains, best_gain, leaf_values, new_predictions.reshape(rows)


def solution(mesh):
    rows = P(("groups", "rows"))
    return jax.shard_map(
        functools.partial(body, mesh),
        mesh=mesh,
        in_specs=(
            P(("groups", "rows"), None),
            rows,
            rows,
            rows,
            rows,
            P("groups"),
            P("groups"),
        ),
        out_specs=(
            P(("groups", "rows"), None, None),
            P("groups"),
            P(None, "groups"),
            rows,
        ),
        check_vma=False,
    )
```

```python
import functools

import jax
import jax.numpy as jnp
from jax import lax
from jax.experimental import pallas as pl
from jax.experimental.pallas import tpu as pltpu
from jax.sharding import PartitionSpec as P

BINS = 256
NODES = 16
LANES = 128
HALF = BINS // 2
EXTRA = 4
QUAD = 4
BLOCK = 16

l2_penalty = 1.0
shrinkage = 0.5

VMEM = pl.BlockSpec(memory_space=pltpu.VMEM)
SMEM = pl.BlockSpec(memory_space=pltpu.SMEM)
PARAMS = pltpu.CompilerParams(vmem_limit_bytes=16 * 1024 * 1024)


def prep_kernel(bins_ref, grad_ref, hess_ref, node_ref, feat_ref, cut_ref, pay_ref, own_ref):
    peers = pay_ref.shape[0]
    rows, feats = bins_ref.shape
    owned = feats // peers
    chunks = rows // LANES
    base = chunks * owned
    node_col = lax.broadcasted_iota(jnp.int32, (NODES, LANES), 0)
    feat_pos = lax.broadcasted_iota(jnp.int32, (NODES, feats), 1)
    node_pos = lax.broadcasted_iota(jnp.int32, (NODES, feats), 0)
    wanted = jnp.zeros((NODES, feats), jnp.int32)
    cut = jnp.zeros((NODES, LANES), jnp.int32)
    for n in range(NODES):
        wanted = jnp.where(node_pos == n, feat_ref[n], wanted)
        cut = jnp.where(node_col == n, cut_ref[n], cut)
    cut = cut.astype(jnp.float32)
    pick = jnp.where(feat_pos == wanted, 1.0, 0.0).astype(jnp.bfloat16)
    for c in range(chunks):
        span = slice(c * LANES, (c + 1) * LANES)
        block = bins_ref[span, :].astype(jnp.float32)
        picked = lax.dot_general(
            pick,
            block.astype(jnp.bfloat16),
            (((1,), (1,)), ((), ())),
            preferred_element_type=jnp.float32,
        )
        node = node_ref[span].reshape(1, LANES)
        member = node == node_col
        side = jnp.sum(
            jnp.where(member & (picked > cut), 1.0, 0.0), axis=0, keepdims=True
        )
        info = [
            grad_ref[span].astype(jnp.float32).reshape(1, LANES),
            hess_ref[span].astype(jnp.float32).reshape(1, LANES),
            node.astype(jnp.float32),
            side,
        ]
        for k in range(EXTRA):
            own_ref[k * chunks + c : k * chunks + c + 1, :] = info[k]
        flipped = block.T
        for d in range(peers):
            pay_ref[d, c * owned : (c + 1) * owned, :] = flipped[d * owned : (d + 1) * owned, :]
    info = own_ref[...]
    for d in range(peers):
        pay_ref[d, base:, :] = info


def weigh(pay_ref, base, chunks, w_ref):
    f32 = jnp.float32
    node_col = lax.broadcasted_iota(jnp.int32, (NODES, LANES), 0).astype(f32)

    def build(s, sums):
        out = list(sums)
        for c in range(chunks):
            g, h, node, side = (
                pay_ref[s, base + k * chunks + c : base + k * chunks + c + 1, :]
                for k in range(EXTRA)
            )
            member = node == node_col
            wg = jnp.where(member, g, 0.0)
            wh = jnp.where(member, h, 0.0)
            w_ref[s, c] = jnp.concatenate([wg, wh], axis=0).astype(jnp.bfloat16)
            left = side < 0.5
            out[0] = out[0] + jnp.where(left, wg, 0.0)
            out[1] = out[1] + jnp.where(left, wh, 0.0)
            out[2] = out[2] + wg
            out[3] = out[3] + wh
        return tuple(out)

    zero = jnp.zeros((NODES, LANES), f32)
    return lax.fori_loop(0, pay_ref.shape[0], build, (zero,) * 4)


def settle(sums, chunks, own_ref, pred_ref, leaf_ref, new_ref):
    left_grad, left_hess, node_grad, node_hess = (
        jnp.sum(x, axis=1, keepdims=True) for x in sums
    )
    node_col = lax.broadcasted_iota(jnp.int32, (NODES, LANES), 0).astype(jnp.float32)
    leaf_left = -left_grad / (left_hess + l2_penalty)
    leaf_right = -(node_grad - left_grad) / (node_hess - left_hess + l2_penalty)
    lane = lax.broadcasted_iota(jnp.int32, (NODES, LANES), 1)
    both = jnp.where(lane == 0, leaf_left, leaf_right)
    both = jnp.concatenate([both, jnp.zeros((LANES - NODES, LANES), jnp.float32)], axis=0)
    leaf_ref[...] = both.T[0:2, 0:NODES]
    for c in range(chunks):
        span = slice(c * LANES, (c + 1) * LANES)
        node = own_ref[2 * chunks + c : 2 * chunks + c + 1, :]
        side = own_ref[3 * chunks + c : 3 * chunks + c + 1, :]
        value = jnp.where(side < 0.5, leaf_left, leaf_right)
        value = jnp.sum(jnp.where(node == node_col, value, 0.0), axis=0, keepdims=True)
        new_ref[span] = pred_ref[span] + shrinkage * value.reshape(LANES)


def sweep(pay_ref, w_ref, owned, chunks, finish, carry):
    f8, i16 = jnp.float8_e4m3fn, jnp.int16
    peers = pay_ref.shape[0]
    block = min(peers, BLOCK)
    quads = owned // QUAD
    group = min(4, quads)
    spot = lax.broadcasted_iota(jnp.int32, (32, LANES), 0)
    steps = [(spot + 32 * i).astype(i16) for i in range(HALF // 32)]
    one = jnp.ones((32, LANES), f8)
    nil = jnp.zeros((32, LANES), f8)
    none = jnp.zeros((NODES, LANES), jnp.bfloat16)

    def terms(s, c, f):
        row = pay_ref[s, pl.ds(c * owned + f, 1), :].astype(jnp.int32)
        bins = jnp.broadcast_to(row, (NODES, LANES)).astype(i16)
        high16 = bins >= i16(HALF)
        low = jnp.where(high16, bins - i16(HALF), bins)
        low = jnp.concatenate([low, low], axis=0)
        rhs = jnp.concatenate([jnp.where(low <= t, one, nil) for t in steps], axis=0)
        wg, wh = w_ref[s, c, 0:NODES, :], w_ref[s, c, NODES : 2 * NODES, :]
        upper = high16
        lhs = jnp.concatenate(
            [
                jnp.where(upper, none, wg),
                jnp.where(upper, none, wh),
                jnp.where(upper, wg, none),
                jnp.where(upper, wh, none),
            ],
            axis=0,
        )
        return lhs, rhs

    def tile(s, t, f):
        part = [[terms(s, 2 * t + i, f + e) for i in range(2)] for e in range(2)]
        return [
            jnp.concatenate(
                [jnp.concatenate([p[k] for p in e], axis=1) for e in part], axis=0
            )
            for k in range(2)
        ]

    def sources(at, q, acc):
        for s in range(block):
            for t in range(chunks // 2):
                reg = (s * (chunks // 2) + t) % 2
                for m in range(2):
                    lhs, rhs = tile(at + s, t, q * QUAD + m * 2)
                    pltpu.matmul_push_rhs(rhs, staging_register=reg, mxu_index=m, transpose=True)
                    pltpu.matmul_acc_lhs(acc[m], lhs, load_staged_rhs=reg)

    def matmuls(q, acc):
        if peers == block:
            sources(0, q, acc)
        else:
            lax.fori_loop(
                0, peers // block, lambda b, x: (sources(b * block, q, acc), x)[1], 0
            )

    def scan(*acc):
        sets = (acc[0:2], acc[2:4])

        def step(j, carry):
            for i in range(group):
                matmuls(j * group + i, sets[i % 2])
                if i:
                    carry = finish(j * group + i - 1, sets[(i - 1) % 2], carry)
            return finish(j * group + group - 1, sets[(group - 1) % 2], carry)

        for a in acc:
            pltpu.matmul_pop(a)
        return lax.fori_loop(0, quads // group, step, carry)

    shape = ((4 * 2 * NODES, BINS), jnp.float32)
    return pl.run_scoped(
        scan, pltpu.ACC(0)(*shape), pltpu.ACC(1)(*shape), pltpu.ACC(0)(*shape), pltpu.ACC(1)(*shape)
    )


def hist_kernel(chunks, pay_ref, own_ref, pred_ref, gains_ref, best_ref, leaf_ref, new_ref, w_ref):
    peers = pay_ref.shape[0]
    owned = gains_ref.shape[0]
    base = chunks * owned
    sums = weigh(pay_ref, base, chunks, w_ref)
    settle(sums, chunks, own_ref, pred_ref, leaf_ref, new_ref)
    def finish(q, acc, best):
        for m in range(2):
            out = pltpu.matmul_pop(acc[m])
            for e in range(2):
                c = out[e * 64 : (e + 1) * 64, e * HALF : (e + 1) * HALF]
                cum_grad, cum_hess = (
                    jnp.concatenate([a, b + a[:, HALF - 1 : HALF]], axis=1)
                    for a, b in ((c[0:16], c[32:48]), (c[16:32], c[48:64]))
                )
                tot_grad = cum_grad[:, BINS - 1 : BINS]
                tot_hess = cum_hess[:, BINS - 1 : BINS]
                gain = 0.5 * (
                    cum_grad * cum_grad / (cum_hess + l2_penalty)
                    + (tot_grad - cum_grad) ** 2 / (tot_hess - cum_hess + l2_penalty)
                    - tot_grad * tot_grad / (tot_hess + l2_penalty)
                )
                gains_ref[q * QUAD + m * 2 + e] = gain
                best = jnp.maximum(best, gain)
        return best

    best = sweep(
        pay_ref, w_ref, owned, chunks, finish, jnp.full((NODES, BINS), -jnp.inf, jnp.float32)
    )
    best = jnp.maximum(best[:, :LANES], best[:, LANES:])
    best = jnp.concatenate([best, jnp.zeros((LANES - NODES, LANES), jnp.float32)], axis=0)
    row = jnp.max(best.T, axis=0, keepdims=True)
    for d in range(peers):
        best_ref[d] = row


def body(mesh, bin_ids, gradients, hessians, node_ids, predictions, split_feature, split_bin):
    peers = mesh.shape["rows"]
    rows, feats = bin_ids.shape
    owned = feats // peers
    chunks = rows // LANES
    f32 = jnp.float32
    depth = chunks * (owned + EXTRA)
    pay, own = pl.pallas_call(
        prep_kernel,
        out_shape=[
            jax.ShapeDtypeStruct((peers, depth, LANES), f32),
            jax.ShapeDtypeStruct((chunks * EXTRA, LANES), f32),
        ],
        in_specs=[VMEM] * 4 + [SMEM] * 2,
        out_specs=[VMEM] * 2,
        name="prep",
    )(bin_ids, gradients, hessians, node_ids, split_feature, split_bin)
    got = lax.all_to_all(pay, "rows", 0, 0, tiled=True)
    gains, best, leaf_values, new_predictions = pl.pallas_call(
        functools.partial(hist_kernel, chunks),
        out_shape=(
            jax.ShapeDtypeStruct((owned, NODES, BINS), f32),
            jax.ShapeDtypeStruct((peers, 1, LANES), f32),
            jax.ShapeDtypeStruct((2, NODES), f32),
            jax.ShapeDtypeStruct((rows,), f32),
        ),
        in_specs=[VMEM] * 3,
        out_specs=(VMEM,) * 4,
        scratch_shapes=[pltpu.VMEM((peers, chunks, 2 * NODES, LANES), jnp.bfloat16)],
        compiler_params=PARAMS,
        name="hist",
    )(got, own, predictions)
    spread = lax.all_to_all(best, "rows", 0, 0, tiled=True)
    best_gain = jnp.max(spread, axis=(0, 1))[:NODES]
    return gains, best_gain, leaf_values, new_predictions


def solution(mesh):
    rows = P(("groups", "rows"))
    return jax.shard_map(
        functools.partial(body, mesh),
        mesh=mesh,
        in_specs=(
            P(("groups", "rows"), None),
            rows,
            rows,
            rows,
            rows,
            P("groups"),
            P("groups"),
        ),
        out_specs=(
            P(("groups", "rows"), None, None),
            P("groups"),
            P(None, "groups"),
            rows,
        ),
        check_vma=False,
    )
```

```python
import functools

import jax
import jax.numpy as jnp
from jax import lax
from jax.experimental import pallas as pl
from jax.experimental.pallas import tpu as pltpu
from jax.sharding import PartitionSpec as P

BINS = 256
NODES = 16
LANES = 128
HALF = BINS // 2
EXTRA = 4
QUAD = 4
BLOCK = 16
MOST_HOPS = 16


l2_penalty = 1.0
shrinkage = 0.5

VMEM = pl.BlockSpec(memory_space=pltpu.VMEM)
HBM = pl.BlockSpec(memory_space=pltpu.HBM)
PARAMS = pltpu.CompilerParams(vmem_limit_bytes=16 * 1024 * 1024)


def hop_order(peers):
    far = list(range(peers - 1, peers // 2 - 1, -1))
    near = list(range(peers // 2 - 1, 0, -1))
    split = max(len(near) - 3, 0)
    return far[:4] + near[split:] + far[4:] + near[:split]


def stage_hops(peers):
    order = [0] + hop_order(peers)
    half, quarter = peers // 2, peers // 4
    return [order[:half], order[half : half + quarter], order[half + quarter :]]


def prep_kernel(peers, bins_hbm, *refs):
    inputs, outs, scratch = refs[:6], refs[6:-10], refs[-10:]
    own_ref, block_refs = outs[0], outs[1:]
    bins_ref, grad_ref, hess_ref, node_ref, pred_ref, feat_ref, cut_ref = scratch[:7]
    pay_ref, bin_sems, sems = scratch[7:]
    rows, feats = bins_ref.shape
    owned = feats // peers
    chunks = rows // LANES
    base = chunks * owned
    small = [
        pltpu.make_async_copy(src, dst, sems.at[i])
        for i, (src, dst) in enumerate(
            zip(inputs, (grad_ref, hess_ref, node_ref, pred_ref, feat_ref, cut_ref))
        )
    ]
    large = [
        pltpu.make_async_copy(
            bins_hbm.at[pl.ds(c * LANES, LANES), :],
            bins_ref.at[pl.ds(c * LANES, LANES), :],
            bin_sems.at[c],
        )
        for c in range(chunks)
    ]
    for copy in small + large:
        copy.start()
    for copy in small:
        copy.wait()
    target = block_refs[0] if peers > MOST_HOPS else pay_ref
    node_col = lax.broadcasted_iota(jnp.int32, (NODES, LANES), 0)
    feat_pos = lax.broadcasted_iota(jnp.int32, (NODES, feats), 1)
    node_pos = lax.broadcasted_iota(jnp.int32, (NODES, feats), 0)
    wanted = jnp.zeros((NODES, feats), jnp.int32)
    cut = jnp.zeros((NODES, LANES), jnp.int32)
    for n in range(NODES):
        wanted = jnp.where(node_pos == n, feat_ref[n], wanted)
        cut = jnp.where(node_col == n, cut_ref[n], cut)
    cut = cut.astype(jnp.float32)
    pick = jnp.where(feat_pos == wanted, 1.0, 0.0).astype(jnp.bfloat16)
    for c in range(chunks):
        large[c].wait()
        span = slice(c * LANES, (c + 1) * LANES)
        block = bins_ref[span, :].astype(jnp.float32)
        picked = lax.dot_general(
            pick,
            block.astype(jnp.bfloat16),
            (((1,), (1,)), ((), ())),
            preferred_element_type=jnp.float32,
        )
        node = node_ref[span].reshape(1, LANES)
        member = node == node_col
        side = jnp.sum(
            jnp.where(member & (picked > cut), 1.0, 0.0), axis=0, keepdims=True
        )
        info = [
            grad_ref[span].astype(jnp.float32).reshape(1, LANES),
            hess_ref[span].astype(jnp.float32).reshape(1, LANES),
            node.astype(jnp.float32),
            side,
            pred_ref[span].reshape(1, LANES),
        ]
        for k in range(EXTRA + 1):
            own_ref[k * chunks + c : k * chunks + c + 1, :] = info[k]
        flipped = block.T
        for d in range(peers):
            target[d, c * owned : (c + 1) * owned, :] = flipped[d * owned : (d + 1) * owned, :]
    info = own_ref[0 : EXTRA * chunks, :]
    if peers > MOST_HOPS:
        for d in range(peers):
            target[d, base:, :] = info
    else:
        me = lax.axis_index("rows")
        for k, block_ref in enumerate(block_refs):
            block_ref[0:base, :] = target[me ^ k, 0:base, :]
            block_ref[base:, :] = info


def weigh(read, s, base, chunks, w_ref, sums):
    node_col = lax.broadcasted_iota(jnp.int32, (NODES, LANES), 0).astype(jnp.float32)
    out = list(sums)
    for c in range(chunks):
        g, h, node, side = (read(s, base + k * chunks + c) for k in range(EXTRA))
        member = node == node_col
        wg = jnp.where(member, g, 0.0)
        wh = jnp.where(member, h, 0.0)
        w_ref[s, c] = jnp.concatenate([wg, wh], axis=0).astype(jnp.bfloat16)
        left = side < 0.5
        out[0] = out[0] + jnp.where(left, wg, 0.0)
        out[1] = out[1] + jnp.where(left, wh, 0.0)
        out[2] = out[2] + wg
        out[3] = out[3] + wh
    return tuple(out)


def weigh_all(read, count, base, chunks, w_ref, sums):
    if count <= MOST_HOPS:
        for s in range(count):
            sums = weigh(read, s, base, chunks, w_ref, sums)
        return sums
    return lax.fori_loop(
        0, count, lambda s, x: weigh(read, s, base, chunks, w_ref, x), tuple(sums)
    )


def no_sums():
    return (jnp.zeros((NODES, LANES), jnp.float32),) * 4


def settle(sums, chunks, own_ref, leaf_ref, new_ref):
    left_grad, left_hess, node_grad, node_hess = (
        jnp.sum(x, axis=1, keepdims=True) for x in sums
    )
    node_col = lax.broadcasted_iota(jnp.int32, (NODES, LANES), 0).astype(jnp.float32)
    leaf_left = -left_grad / (left_hess + l2_penalty)
    leaf_right = -(node_grad - left_grad) / (node_hess - left_hess + l2_penalty)
    lane = lax.broadcasted_iota(jnp.int32, (NODES, LANES), 1)
    both = jnp.where(lane == 0, leaf_left, leaf_right)
    both = jnp.concatenate([both, jnp.zeros((LANES - NODES, LANES), jnp.float32)], axis=0)
    leaf_ref[...] = both.T[0:2, 0:NODES]
    for c in range(chunks):
        span = slice(c * LANES, (c + 1) * LANES)
        node = own_ref[2 * chunks + c : 2 * chunks + c + 1, :]
        side = own_ref[3 * chunks + c : 3 * chunks + c + 1, :]
        value = jnp.where(side < 0.5, leaf_left, leaf_right)
        value = jnp.sum(jnp.where(node == node_col, value, 0.0), axis=0, keepdims=True)
        pred = own_ref[EXTRA * chunks + c : EXTRA * chunks + c + 1, :]
        new_ref[span] = (pred + shrinkage * value).reshape(LANES)


def sweep(read, count, w_ref, owned, chunks, finish, carry):
    f8, i16 = jnp.float8_e4m3fn, jnp.int16
    block = min(count, BLOCK)
    quads = owned // QUAD
    group = min(4, quads)
    spot = lax.broadcasted_iota(jnp.int32, (32, LANES), 0)
    steps = [(spot + 32 * i).astype(i16) for i in range(HALF // 32)]
    one = jnp.ones((32, LANES), f8)
    nil = jnp.zeros((32, LANES), f8)
    none = jnp.zeros((NODES, LANES), jnp.bfloat16)

    def terms(s, c, f):
        row = read(s, c * owned + f).astype(jnp.int32)
        bins = jnp.broadcast_to(row, (NODES, LANES)).astype(i16)
        high16 = bins >= i16(HALF)
        low = jnp.where(high16, bins - i16(HALF), bins)
        low = jnp.concatenate([low, low], axis=0)
        rhs = jnp.concatenate([jnp.where(low <= t, one, nil) for t in steps], axis=0)
        wg, wh = w_ref[s, c, 0:NODES, :], w_ref[s, c, NODES : 2 * NODES, :]
        upper = high16
        lhs = jnp.concatenate(
            [
                jnp.where(upper, none, wg),
                jnp.where(upper, none, wh),
                jnp.where(upper, wg, none),
                jnp.where(upper, wh, none),
            ],
            axis=0,
        )
        return lhs, rhs

    def tile(s, t, f):
        part = [[terms(s, 2 * t + i, f + e) for i in range(2)] for e in range(2)]
        return [
            jnp.concatenate(
                [jnp.concatenate([p[k] for p in e], axis=1) for e in part], axis=0
            )
            for k in range(2)
        ]

    def sources(at, q, acc):
        for s in range(block):
            for t in range(chunks // 2):
                reg = (s * (chunks // 2) + t) % 2
                for m in range(2):
                    lhs, rhs = tile(at + s, t, q * QUAD + m * 2)
                    pltpu.matmul_push_rhs(rhs, staging_register=reg, mxu_index=m, transpose=True)
                    pltpu.matmul_acc_lhs(acc[m], lhs, load_staged_rhs=reg)

    def matmuls(q, acc):
        if count == block:
            sources(0, q, acc)
        else:
            lax.fori_loop(
                0, count // block, lambda b, x: (sources(b * block, q, acc), x)[1], 0
            )

    def scan(*acc):
        sets = (acc[0:2], acc[2:4])

        def step(j, carry):
            for i in range(group):
                matmuls(j * group + i, sets[i % 2])
                if i:
                    carry = finish(j * group + i - 1, sets[(i - 1) % 2], carry)
            return finish(j * group + group - 1, sets[(group - 1) % 2], carry)

        for a in acc:
            pltpu.matmul_pop(a)
        return lax.fori_loop(0, quads // group, step, carry)

    shape = ((4 * 2 * NODES, BINS), jnp.float32)
    return pl.run_scoped(
        scan, pltpu.ACC(0)(*shape), pltpu.ACC(1)(*shape), pltpu.ACC(0)(*shape), pltpu.ACC(1)(*shape)
    )


def reader(refs):
    if len(refs) == 1:
        return lambda s, r: refs[0][s, pl.ds(r, 1), :]
    return lambda s, r: refs[s][pl.ds(r, 1), :]


def stage_kernel(chunks, sources, *refs):
    block_refs, before, (part_ref, sums_ref, w_ref) = refs[:sources], refs[sources:-3], refs[-3:]
    owned = part_ref.shape[0]
    read = reader(block_refs)
    sums = tuple(before[1][k] for k in range(4)) if before else no_sums()
    sums = weigh_all(read, sources, chunks * owned, chunks, w_ref, sums)
    for k in range(4):
        sums_ref[k] = sums[k]

    def finish(q, acc, carry):
        for m in range(2):
            out = pltpu.matmul_pop(acc[m])
            for e in range(2):
                f = q * QUAD + m * 2 + e
                c = out[e * 64 : (e + 1) * 64, e * HALF : (e + 1) * HALF]
                part_ref[f] = c + before[0][f] if before else c
        return carry

    sweep(read, sources, w_ref, owned, chunks, finish, 0)


def last_kernel(chunks, split, *refs):
    gains_ref, best_ref, leaf_ref, new_ref, w_ref = refs[-5:]
    own_ref = refs[-6]
    block_refs = refs[:-6]
    sums = no_sums()
    if split:
        part_ref, sums_ref = refs[-8:-6]
        block_refs = refs[:-8]
        sums = tuple(sums_ref[k] for k in range(4))
    peers = best_ref.shape[0]
    owned = gains_ref.shape[0]
    read = reader(block_refs)
    count = len(block_refs) if len(block_refs) > 1 else peers
    sums = weigh_all(read, count, chunks * owned, chunks, w_ref, sums)
    settle(sums, chunks, own_ref, leaf_ref, new_ref)

    def finish(q, acc, best):
        for m in range(2):
            out = pltpu.matmul_pop(acc[m])
            for e in range(2):
                c = out[e * 64 : (e + 1) * 64, e * HALF : (e + 1) * HALF]
                if split:
                    c = c + part_ref[q * QUAD + m * 2 + e]
                cum_grad, cum_hess = (
                    jnp.concatenate([a, b + a[:, HALF - 1 : HALF]], axis=1)
                    for a, b in ((c[0:16], c[32:48]), (c[16:32], c[48:64]))
                )
                tot_grad = cum_grad[:, BINS - 1 : BINS]
                tot_hess = cum_hess[:, BINS - 1 : BINS]
                gain = 0.5 * (
                    cum_grad * cum_grad / (cum_hess + l2_penalty)
                    + (tot_grad - cum_grad) ** 2 / (tot_hess - cum_hess + l2_penalty)
                    - tot_grad * tot_grad / (tot_hess + l2_penalty)
                )
                gains_ref[q * QUAD + m * 2 + e] = gain
                best = jnp.maximum(best, gain)
        return best

    least = jnp.full((NODES, BINS), -jnp.inf, jnp.float32)
    best = sweep(read, count, w_ref, owned, chunks, finish, least)
    best = jnp.maximum(best[:, :LANES], best[:, LANES:])
    best = jnp.concatenate([best, jnp.zeros((LANES - NODES, LANES), jnp.float32)], axis=0)
    row = jnp.max(best.T, axis=0, keepdims=True)
    for d in range(peers):
        best_ref[d] = row


def body(mesh, bin_ids, gradients, hessians, node_ids, predictions, split_feature, split_bin):
    peers = mesh.shape["rows"]
    rows, feats = bin_ids.shape
    owned = feats // peers
    chunks = rows // LANES
    f32 = jnp.float32
    depth = chunks * (owned + EXTRA)
    hops = hop_order(peers) if peers <= MOST_HOPS else []
    many = jax.ShapeDtypeStruct((peers, depth, LANES), f32)
    single = jax.ShapeDtypeStruct((depth, LANES), f32)

    def cost(sources):
        work = 2 * sources * rows * owned * 2 * NODES * BINS
        return pl.CostEstimate(flops=work, bytes_accessed=work // 4096, transcendentals=0)

    def weights(sources):
        return pltpu.VMEM((sources, chunks, 2 * NODES, LANES), jnp.bfloat16)

    own, *blocks = pl.pallas_call(
        functools.partial(prep_kernel, peers),
        out_shape=[jax.ShapeDtypeStruct((chunks * (EXTRA + 1), LANES), f32)]
        + ([single] * peers if hops else [many]),
        in_specs=[HBM] * 7,
        out_specs=[VMEM] * (1 + (peers if hops else 1)),
        scratch_shapes=[
            pltpu.VMEM((rows, feats), jnp.int32),
            pltpu.VMEM((rows,), gradients.dtype),
            pltpu.VMEM((rows,), hessians.dtype),
            pltpu.VMEM((rows,), jnp.int32),
            pltpu.VMEM((rows,), f32),
            pltpu.SMEM((NODES,), jnp.int32),
            pltpu.SMEM((NODES,), jnp.int32),
            pltpu.VMEM((peers if hops else 1, depth, LANES), f32),
            pltpu.SemaphoreType.DMA((chunks,)),
            pltpu.SemaphoreType.DMA((6,)),
        ],
        name="prep",
    )(bin_ids, gradients, hessians, node_ids, predictions, split_feature, split_bin)
    if hops:
        landed = {0: blocks[0]}
        for k in hops:
            landed[k] = lax.ppermute(
                blocks[k], "rows", [(i, i ^ k) for i in range(peers)]
            )
        part = []
        stages = stage_hops(peers)
        for group in stages[:-1]:
            part = pl.pallas_call(
                functools.partial(stage_kernel, chunks, len(group)),
                out_shape=(
                    jax.ShapeDtypeStruct((owned, 4 * NODES, HALF), f32),
                    jax.ShapeDtypeStruct((4, NODES, LANES), f32),
                ),
                in_specs=[VMEM] * (len(group) + len(part)),
                out_specs=(VMEM, VMEM),
                scratch_shapes=[weights(len(group))],
                compiler_params=PARAMS,
                cost_estimate=cost(len(group)),
            )(*[landed[k] for k in group], *part)
        late = stages[-1]
        operands = [landed[k] for k in late] + list(part)
    else:
        operands = [lax.all_to_all(blocks[0], "rows", 0, 0, tiled=True)]
    count = len(late) if hops else peers
    gains, best, leaf_values, new_predictions = pl.pallas_call(
        functools.partial(last_kernel, chunks, bool(hops)),
        out_shape=(
            jax.ShapeDtypeStruct((owned, NODES, BINS), f32),
            jax.ShapeDtypeStruct((peers, 1, LANES), f32),
            jax.ShapeDtypeStruct((2, NODES), f32),
            jax.ShapeDtypeStruct((rows,), f32),
        ),
        in_specs=[VMEM] * (len(operands) + 1),
        out_specs=(VMEM,) * 4,
        scratch_shapes=[weights(count)],
        compiler_params=PARAMS,
        cost_estimate=cost(count),
        name="hist",
    )(*operands, own)
    spread = lax.all_to_all(best, "rows", 0, 0, tiled=True)
    best_gain = jnp.max(spread, axis=(0, 1))[:NODES]
    return gains, best_gain, leaf_values, new_predictions


def solution(mesh):
    rows = P(("groups", "rows"))
    return jax.shard_map(
        functools.partial(body, mesh),
        mesh=mesh,
        in_specs=(
            P(("groups", "rows"), None),
            rows,
            rows,
            rows,
            rows,
            P("groups"),
            P("groups"),
        ),
        out_specs=(
            P(("groups", "rows"), None, None),
            P("groups"),
            P(None, "groups"),
            rows,
        ),
        check_vma=False,
    )
```

```python
import functools

import jax
import jax.numpy as jnp
from jax import lax
from jax.experimental import pallas as pl
from jax.experimental.pallas import tpu as pltpu
from jax.sharding import PartitionSpec as P

BINS = 256
NODES = 16
LANES = 128
HALF = BINS // 2
EXTRA = 4
QUAD = 4
BLOCK = 16
MOST_HOPS = 16


l2_penalty = 1.0
shrinkage = 0.5

VMEM = pl.BlockSpec(memory_space=pltpu.VMEM)
HBM = pl.BlockSpec(memory_space=pltpu.HBM)
PARAMS = pltpu.CompilerParams(vmem_limit_bytes=16 * 1024 * 1024)


def hop_order(peers):
    far = list(range(peers - 1, peers // 2 - 1, -1))
    near = list(range(peers // 2 - 1, 0, -1))
    split = max(len(near) - 3, 0)
    return far[:4] + near[split:] + far[4:5] + near[:split] + far[5:]


def stage_hops(peers):
    order = [0] + hop_order(peers)
    early, late = peers // 2, max(peers * 13 // 16, peers // 2 + 1)
    return [order[:early], order[early:late], order[late:]]


def prep_kernel(peers, bins_hbm, *refs):
    inputs, outs, scratch = refs[:6], refs[6:-10], refs[-10:]
    own_ref, block_refs = outs[0], outs[1:]
    bins_ref, grad_ref, hess_ref, node_ref, pred_ref, feat_ref, cut_ref = scratch[:7]
    pay_ref, bin_sems, sems = scratch[7:]
    rows, feats = bins_ref.shape
    owned = feats // peers
    chunks = rows // LANES
    base = chunks * owned
    small = [
        pltpu.make_async_copy(src, dst, sems.at[i])
        for i, (src, dst) in enumerate(
            zip(inputs, (grad_ref, hess_ref, node_ref, pred_ref, feat_ref, cut_ref))
        )
    ]
    large = [
        pltpu.make_async_copy(
            bins_hbm.at[pl.ds(c * LANES, LANES), :],
            bins_ref.at[pl.ds(c * LANES, LANES), :],
            bin_sems.at[c],
        )
        for c in range(chunks)
    ]
    for copy in small + large:
        copy.start()
    for copy in small:
        copy.wait()
    target = block_refs[0] if peers > MOST_HOPS else pay_ref
    node_col = lax.broadcasted_iota(jnp.int32, (NODES, LANES), 0)
    feat_pos = lax.broadcasted_iota(jnp.int32, (NODES, feats), 1)
    node_pos = lax.broadcasted_iota(jnp.int32, (NODES, feats), 0)
    wanted = jnp.zeros((NODES, feats), jnp.int32)
    cut = jnp.zeros((NODES, LANES), jnp.int32)
    for n in range(NODES):
        wanted = jnp.where(node_pos == n, feat_ref[n], wanted)
        cut = jnp.where(node_col == n, cut_ref[n], cut)
    cut = cut.astype(jnp.float32)
    pick = jnp.where(feat_pos == wanted, 1.0, 0.0).astype(jnp.bfloat16)
    for c in range(chunks):
        large[c].wait()
        span = slice(c * LANES, (c + 1) * LANES)
        block = bins_ref[span, :].astype(jnp.float32)
        picked = lax.dot_general(
            pick,
            block.astype(jnp.bfloat16),
            (((1,), (1,)), ((), ())),
            preferred_element_type=jnp.float32,
        )
        node = node_ref[span].reshape(1, LANES)
        member = node == node_col
        side = jnp.sum(
            jnp.where(member & (picked > cut), 1.0, 0.0), axis=0, keepdims=True
        )
        info = [
            grad_ref[span].astype(jnp.float32).reshape(1, LANES),
            hess_ref[span].astype(jnp.float32).reshape(1, LANES),
            node.astype(jnp.float32),
            side,
            pred_ref[span].reshape(1, LANES),
        ]
        for k in range(EXTRA + 1):
            own_ref[k * chunks + c : k * chunks + c + 1, :] = info[k]
        flipped = block.T
        for d in range(peers):
            target[d, c * owned : (c + 1) * owned, :] = flipped[d * owned : (d + 1) * owned, :]
    info = own_ref[0 : EXTRA * chunks, :]
    if peers > MOST_HOPS:
        for d in range(peers):
            target[d, base:, :] = info
    else:
        me = lax.axis_index("rows")
        for k, block_ref in enumerate(block_refs):
            block_ref[0:base, :] = target[me ^ k, 0:base, :]
            block_ref[base:, :] = info


def weigh(read, s, base, chunks, w_ref, sums):
    node_col = lax.broadcasted_iota(jnp.int32, (NODES, LANES), 0).astype(jnp.float32)
    out = list(sums)
    for c in range(chunks):
        g, h, node, side = (read(s, base + k * chunks + c) for k in range(EXTRA))
        member = node == node_col
        wg = jnp.where(member, g, 0.0)
        wh = jnp.where(member, h, 0.0)
        w_ref[s, c] = jnp.concatenate([wg, wh], axis=0).astype(jnp.bfloat16)
        left = side < 0.5
        out[0] = out[0] + jnp.where(left, wg, 0.0)
        out[1] = out[1] + jnp.where(left, wh, 0.0)
        out[2] = out[2] + wg
        out[3] = out[3] + wh
    return tuple(out)


def weigh_all(read, count, base, chunks, w_ref, sums):
    if count <= MOST_HOPS:
        for s in range(count):
            sums = weigh(read, s, base, chunks, w_ref, sums)
        return sums
    return lax.fori_loop(
        0, count, lambda s, x: weigh(read, s, base, chunks, w_ref, x), tuple(sums)
    )


def no_sums():
    return (jnp.zeros((NODES, LANES), jnp.float32),) * 4


def settle(sums, chunks, own_ref, leaf_ref, new_ref):
    left_grad, left_hess, node_grad, node_hess = (
        jnp.sum(x, axis=1, keepdims=True) for x in sums
    )
    node_col = lax.broadcasted_iota(jnp.int32, (NODES, LANES), 0).astype(jnp.float32)
    leaf_left = -left_grad / (left_hess + l2_penalty)
    leaf_right = -(node_grad - left_grad) / (node_hess - left_hess + l2_penalty)
    lane = lax.broadcasted_iota(jnp.int32, (NODES, LANES), 1)
    both = jnp.where(lane == 0, leaf_left, leaf_right)
    both = jnp.concatenate([both, jnp.zeros((LANES - NODES, LANES), jnp.float32)], axis=0)
    leaf_ref[...] = both.T[0:2, 0:NODES]
    for c in range(chunks):
        span = slice(c * LANES, (c + 1) * LANES)
        node = own_ref[2 * chunks + c : 2 * chunks + c + 1, :]
        side = own_ref[3 * chunks + c : 3 * chunks + c + 1, :]
        value = jnp.where(side < 0.5, leaf_left, leaf_right)
        value = jnp.sum(jnp.where(node == node_col, value, 0.0), axis=0, keepdims=True)
        pred = own_ref[EXTRA * chunks + c : EXTRA * chunks + c + 1, :]
        new_ref[span] = (pred + shrinkage * value).reshape(LANES)


def sweep(read, count, w_ref, owned, chunks, finish, carry):
    f8, i16 = jnp.float8_e4m3fn, jnp.int16
    block = min(count, BLOCK)
    quads = owned // QUAD
    group = min(quads, 8 if count <= 4 else 4)
    spot = lax.broadcasted_iota(jnp.int32, (32, LANES), 0)
    steps = [(spot + 32 * i).astype(i16) for i in range(HALF // 32)]
    one = jnp.ones((32, LANES), f8)
    nil = jnp.zeros((32, LANES), f8)
    none = jnp.zeros((NODES, LANES), jnp.bfloat16)

    def terms(s, c, f):
        row = read(s, c * owned + f).astype(jnp.int32)
        bins = jnp.broadcast_to(row, (NODES, LANES)).astype(i16)
        high16 = bins >= i16(HALF)
        low = jnp.where(high16, bins - i16(HALF), bins)
        low = jnp.concatenate([low, low], axis=0)
        rhs = jnp.concatenate([jnp.where(low <= t, one, nil) for t in steps], axis=0)
        wg, wh = w_ref[s, c, 0:NODES, :], w_ref[s, c, NODES : 2 * NODES, :]
        upper = high16
        lhs = jnp.concatenate(
            [
                jnp.where(upper, none, wg),
                jnp.where(upper, none, wh),
                jnp.where(upper, wg, none),
                jnp.where(upper, wh, none),
            ],
            axis=0,
        )
        return lhs, rhs

    def tile(s, t, f):
        part = [[terms(s, 2 * t + i, f + e) for i in range(2)] for e in range(2)]
        return [
            jnp.concatenate(
                [jnp.concatenate([p[k] for p in e], axis=1) for e in part], axis=0
            )
            for k in range(2)
        ]

    def sources(at, q, acc):
        for s in range(block):
            for t in range(chunks // 2):
                reg = (s * (chunks // 2) + t) % 2
                for m in range(2):
                    lhs, rhs = tile(at + s, t, q * QUAD + m * 2)
                    pltpu.matmul_push_rhs(rhs, staging_register=reg, mxu_index=m, transpose=True)
                    pltpu.matmul_acc_lhs(acc[m], lhs, load_staged_rhs=reg)

    def matmuls(q, acc):
        if count == block:
            sources(0, q, acc)
        else:
            lax.fori_loop(
                0, count // block, lambda b, x: (sources(b * block, q, acc), x)[1], 0
            )

    def scan(*acc):
        sets = (acc[0:2], acc[2:4])

        def step(j, carry):
            for i in range(group):
                matmuls(j * group + i, sets[i % 2])
                if i:
                    carry = finish(j * group + i - 1, sets[(i - 1) % 2], carry)
            return finish(j * group + group - 1, sets[(group - 1) % 2], carry)

        for a in acc:
            pltpu.matmul_pop(a)
        if quads == group:
            return step(0, carry)
        return lax.fori_loop(0, quads // group, step, carry)

    shape = ((4 * 2 * NODES, BINS), jnp.float32)
    return pl.run_scoped(
        scan, pltpu.ACC(0)(*shape), pltpu.ACC(1)(*shape), pltpu.ACC(0)(*shape), pltpu.ACC(1)(*shape)
    )


def reader(refs):
    if len(refs) == 1:
        return lambda s, r: refs[0][s, pl.ds(r, 1), :]
    return lambda s, r: refs[s][pl.ds(r, 1), :]


def stage_kernel(chunks, sources, *refs):
    block_refs, before, (part_ref, sums_ref, w_ref) = refs[:sources], refs[sources:-3], refs[-3:]
    owned = part_ref.shape[0]
    read = reader(block_refs)
    sums = tuple(before[1][k] for k in range(4)) if before else no_sums()
    sums = weigh_all(read, sources, chunks * owned, chunks, w_ref, sums)
    for k in range(4):
        sums_ref[k] = sums[k]

    def finish(q, acc, carry):
        for m in range(2):
            out = pltpu.matmul_pop(acc[m])
            for e in range(2):
                f = q * QUAD + m * 2 + e
                c = out[e * 64 : (e + 1) * 64, e * HALF : (e + 1) * HALF]
                part_ref[f] = c + before[0][f] if before else c
        return carry

    sweep(read, sources, w_ref, owned, chunks, finish, 0)


def last_kernel(chunks, split, *refs):
    gains_ref, best_ref, leaf_ref, new_ref, w_ref = refs[-5:]
    own_ref = refs[-6]
    block_refs = refs[:-6]
    sums = no_sums()
    if split:
        part_ref, sums_ref = refs[-8:-6]
        block_refs = refs[:-8]
        sums = tuple(sums_ref[k] for k in range(4))
    peers = best_ref.shape[0]
    owned = gains_ref.shape[0]
    read = reader(block_refs)
    count = len(block_refs) if len(block_refs) > 1 else peers
    sums = weigh_all(read, count, chunks * owned, chunks, w_ref, sums)

    def finish(q, acc, best):
        for m in range(2):
            out = pltpu.matmul_pop(acc[m])
            for e in range(2):
                c = out[e * 64 : (e + 1) * 64, e * HALF : (e + 1) * HALF]
                if split:
                    c = c + part_ref[q * QUAD + m * 2 + e]
                cum_grad, cum_hess = (
                    jnp.concatenate([a, b + a[:, HALF - 1 : HALF]], axis=1)
                    for a, b in ((c[0:16], c[32:48]), (c[16:32], c[48:64]))
                )
                tot_grad = cum_grad[:, BINS - 1 : BINS]
                tot_hess = cum_hess[:, BINS - 1 : BINS]
                gain = 0.5 * (
                    cum_grad * cum_grad / (cum_hess + l2_penalty)
                    + (tot_grad - cum_grad) ** 2 / (tot_hess - cum_hess + l2_penalty)
                    - tot_grad * tot_grad / (tot_hess + l2_penalty)
                )
                gains_ref[q * QUAD + m * 2 + e] = gain
                best = jnp.maximum(best, gain)
        return best

    least = jnp.full((NODES, BINS), -jnp.inf, jnp.float32)
    best = sweep(read, count, w_ref, owned, chunks, finish, least)
    settle(sums, chunks, own_ref, leaf_ref, new_ref)
    best = jnp.maximum(best[:, :LANES], best[:, LANES:])
    best = jnp.concatenate([best, jnp.zeros((LANES - NODES, LANES), jnp.float32)], axis=0)
    row = jnp.max(best.T, axis=0, keepdims=True)
    for d in range(peers):
        best_ref[d] = row


def body(mesh, bin_ids, gradients, hessians, node_ids, predictions, split_feature, split_bin):
    peers = mesh.shape["rows"]
    rows, feats = bin_ids.shape
    owned = feats // peers
    chunks = rows // LANES
    f32 = jnp.float32
    depth = chunks * (owned + EXTRA)
    hops = hop_order(peers) if peers <= MOST_HOPS else []
    many = jax.ShapeDtypeStruct((peers, depth, LANES), f32)
    single = jax.ShapeDtypeStruct((depth, LANES), f32)

    def cost(sources):
        work = 2 * sources * rows * owned * 2 * NODES * BINS
        return pl.CostEstimate(flops=work, bytes_accessed=work // 4096, transcendentals=0)

    def weights(sources):
        return pltpu.VMEM((sources, chunks, 2 * NODES, LANES), jnp.bfloat16)

    own, *blocks = pl.pallas_call(
        functools.partial(prep_kernel, peers),
        out_shape=[jax.ShapeDtypeStruct((chunks * (EXTRA + 1), LANES), f32)]
        + ([single] * peers if hops else [many]),
        in_specs=[HBM] * 7,
        out_specs=[VMEM] * (1 + (peers if hops else 1)),
        scratch_shapes=[
            pltpu.VMEM((rows, feats), jnp.int32),
            pltpu.VMEM((rows,), gradients.dtype),
            pltpu.VMEM((rows,), hessians.dtype),
            pltpu.VMEM((rows,), jnp.int32),
            pltpu.VMEM((rows,), f32),
            pltpu.SMEM((NODES,), jnp.int32),
            pltpu.SMEM((NODES,), jnp.int32),
            pltpu.VMEM((peers if hops else 1, depth, LANES), f32),
            pltpu.SemaphoreType.DMA((chunks,)),
            pltpu.SemaphoreType.DMA((6,)),
        ],
        name="prep",
    )(bin_ids, gradients, hessians, node_ids, predictions, split_feature, split_bin)
    if hops:
        landed = {0: blocks[0]}
        for k in hops:
            landed[k] = lax.ppermute(
                blocks[k], "rows", [(i, i ^ k) for i in range(peers)]
            )
        part = []
        stages = stage_hops(peers)
        for group in stages[:-1]:
            part = pl.pallas_call(
                functools.partial(stage_kernel, chunks, len(group)),
                out_shape=(
                    jax.ShapeDtypeStruct((owned, 4 * NODES, HALF), f32),
                    jax.ShapeDtypeStruct((4, NODES, LANES), f32),
                ),
                in_specs=[VMEM] * (len(group) + len(part)),
                out_specs=(VMEM, VMEM),
                scratch_shapes=[weights(len(group))],
                compiler_params=PARAMS,
                cost_estimate=cost(len(group)),
            )(*[landed[k] for k in group], *part)
        late = stages[-1]
        operands = [landed[k] for k in late] + list(part)
    else:
        operands = [lax.all_to_all(blocks[0], "rows", 0, 0, tiled=True)]
    count = len(late) if hops else peers
    gains, best, leaf_values, new_predictions = pl.pallas_call(
        functools.partial(last_kernel, chunks, bool(hops)),
        out_shape=(
            jax.ShapeDtypeStruct((owned, NODES, BINS), f32),
            jax.ShapeDtypeStruct((peers, 1, LANES), f32),
            jax.ShapeDtypeStruct((2, NODES), f32),
            jax.ShapeDtypeStruct((rows,), f32),
        ),
        in_specs=[VMEM] * (len(operands) + 1),
        out_specs=(VMEM,) * 4,
        scratch_shapes=[weights(count)],
        compiler_params=PARAMS,
        cost_estimate=cost(count),
        name="hist",
    )(*operands, own)
    spread = lax.all_to_all(best, "rows", 0, 0, tiled=True)
    best_gain = jnp.max(spread, axis=(0, 1))[:NODES]
    return gains, best_gain, leaf_values, new_predictions


def solution(mesh):
    rows = P(("groups", "rows"))
    return jax.shard_map(
        functools.partial(body, mesh),
        mesh=mesh,
        in_specs=(
            P(("groups", "rows"), None),
            rows,
            rows,
            rows,
            rows,
            P("groups"),
            P("groups"),
        ),
        out_specs=(
            P(("groups", "rows"), None, None),
            P("groups"),
            P(None, "groups"),
            rows,
        ),
        check_vma=False,
    )
```
